32 devices in a mesh: member: 2 (over y), lat: 4 (over z), lon: 2 (over x), lev: 2 (over core).
Axes of the slice: x: 2, y: 2, z: 4, core: 2. Of those that a mesh axis runs over, the one named last changes fastest.
Arguments:
- perturbation: bfloat16 [4, 64, 16, 8, 128], P('member', 'lev', 'lat', 'lon'), parts along dimension 0, may hold values from -6 to 6
- adjoint_forcing: bfloat16 [4, 64, 16, 8, 128], P('member', 'lev', 'lat', 'lon'), parts along dimension 0, may hold values from -6 to 6
- source_rows: int32 [16, 8, 4], P('lat', 'lon'), may hold values from 0 to 15, as said below
- source_cols: int32 [16, 8, 4], P('lat', 'lon'), may hold values from 0 to 7, as said below
- cubic_weights: bfloat16 [16, 8, 4, 128, 128], P('lat', 'lon'), may hold values from -1.5 to 1.5
Outputs:
- tangent_out: bfloat16 [4, 64, 16, 8, 128], P('member', 'lev', 'lat', 'lon'), parts along dimension 0
- adjoint_out: bfloat16 [4, 64, 16, 8, 128], P('member', 'lev', 'lat', 'lon'), parts along dimension 0
The draws below stay inside these ranges and needn't reach their ends.
There are 2 independent parts, one for each index of `member`. The reference program is written for one: setup_inputs(seed, part) draws one part's arguments, and reference() takes and returns one part's arrays. A program takes and returns all parts, laid end to end along the dimension named above; an argument that names none is the same for every part. Nothing has to cross between parts.
Inputs may be any that keep to these rules, and one draw needn't show every extreme that they name: source_rows[i, j, k] differs from i by at most 8. source_cols[i, j, k] is j + d modulo 8 with d from -1 to 1, and from -2 to 2 where i lies in the first or last 4 block rows.
All inputs are finite; a program needn't handle non-finite values.
Results may differ from the reference program's by a relative error of at most 0.004.
Values may be sent and summed in bfloat16 or wider, within the bound.
A program may use at most 64 MiB of HBM per device.

```python
import math
import jax
import jax.numpy as jnp
from jax import lax

CELLS = 128
STENCIL = 4
BAND_ROWS = 4
FIELDS = 2
LEVELS = 64
LAT_ROWS = 16
LON_COLS = 8
N_LAT = 4


def draw_source_rows(key, part):
    first_key, second_key = jax.random.split(jax.random.fold_in(key, 11))
    row_ids = jnp.arange(LAT_ROWS, dtype=jnp.int32)[:, None, None]
    reach_rows = 2 * BAND_ROWS
    shape = (LAT_ROWS, LON_COLS, STENCIL)
    offsets = jax.random.randint(first_key, shape, -reach_rows, reach_rows + 1)
    signs = 2 * jax.random.randint(second_key, shape, 0, 2) - 1
    last_one = jnp.arange(STENCIL, dtype=jnp.int32)[None, None, :] == STENCIL - 1
    offsets = jnp.where(last_one, signs * reach_rows, offsets)
    return jnp.clip(row_ids + offsets, 0, LAT_ROWS - 1).astype(jnp.int32)


def draw_source_cols(key, part):
    first_key, second_key = jax.random.split(jax.random.fold_in(key, 23))
    row_ids = jnp.arange(LAT_ROWS, dtype=jnp.int32)[:, None, None]
    band_ids = row_ids // BAND_ROWS
    polar = (band_ids == 0) | (band_ids == N_LAT - 1)
    reach_cols = jnp.where(polar, 2, 1)
    col_ids = jnp.arange(LON_COLS, dtype=jnp.int32)[None, :, None]
    shape = (LAT_ROWS, LON_COLS, STENCIL)
    offsets = jax.random.randint(first_key, shape, -2, 3)
    offsets = jnp.clip(offsets, -reach_cols, reach_cols)
    signs = 2 * jax.random.randint(second_key, shape, 0, 2) - 1
    last_one = jnp.arange(STENCIL, dtype=jnp.int32)[None, None, :] == STENCIL - 1
    offsets = jnp.where(last_one & polar, signs * 2, offsets)
    return jnp.mod(col_ids + offsets, LON_COLS).astype(jnp.int32)


def draw_cubic_weights(key, part):
    second_key = jax.random.fold_in(jax.random.fold_in(key, 37), 1)
    identity = jnp.eye(CELLS, dtype=jnp.float32)
    diagonal = jnp.full((LAT_ROWS, LON_COLS, STENCIL, 1, 1), 0.5, jnp.float32)
    noise = jax.random.normal(second_key, (LAT_ROWS, LON_COLS, STENCIL, CELLS, CELLS), jnp.float32)
    noise = jnp.clip(noise * (0.35 / math.sqrt(CELLS)), -0.6, 0.6)
    return (diagonal * identity + noise).astype(jnp.bfloat16)


def steps_of(rng, shape, shards, least, largest):
    loudness, own = 1.0, jax.random.fold_in(rng, 6)
    for axis_at, blocks in shards:
        draws = jnp.exp(jax.random.uniform(jax.random.fold_in(own, axis_at), (blocks,), jnp.float32, least / len(shards), largest / len(shards)))
        loudness = loudness * jnp.repeat(draws, shape[axis_at] // blocks).reshape([-1 if axis == axis_at else 1 for axis in range(len(shape))])
    return loudness


def centred(key, shape, scale, reach, cuts=(), kind=jnp.bfloat16):
    drawn = scale * jax.random.normal(key, shape, jnp.float32)
    if cuts:
        drawn = drawn * steps_of(key, shape, cuts, -0.22, 0.18)
    return jnp.clip(drawn, -reach, reach).astype(kind)


def setup_inputs(seed: int = 0, part: int = 0) -> dict:
    arg_keys = jax.random.split(jax.random.key(seed), 6)
    part_splits = jax.random.split(jax.random.fold_in(arg_keys[5], part), 6)
    return {
        "perturbation": centred(part_splits[0], (FIELDS, LEVELS, LAT_ROWS, LON_COLS, CELLS), 1.0, 6.0, ((1, 2), (2, 4), (3, 2))),
        "adjoint_forcing": centred(part_splits[1], (FIELDS, LEVELS, LAT_ROWS, LON_COLS, CELLS), 1.0, 6.0, ((1, 2), (2, 4), (3, 2))),
        "source_rows": draw_source_rows(jax.random.fold_in(arg_keys[5], 71), part),
        "source_cols": draw_source_cols(jax.random.fold_in(arg_keys[5], 71), part),
        "cubic_weights": draw_cubic_weights(jax.random.fold_in(arg_keys[5], 71), part),
    }


def interpolate(field, source_rows, source_cols, cubic_weights):

    def one_row(pieces):
        rows_here, cols_here, weights_here = pieces
        picked = field[:, :, rows_here, cols_here, :]
        return jnp.einsum('flnks,nksc->flnc', picked, weights_here.astype(jnp.float32), precision=lax.Precision.HIGHEST)
    mapped = lax.map(one_row, (source_rows, source_cols, cubic_weights))
    return jnp.transpose(mapped, (1, 2, 0, 3, 4))

def reference(perturbation, adjoint_forcing, source_rows, source_cols, cubic_weights):

    def linear_map(field):
        return interpolate(field, source_rows, source_cols, cubic_weights)
    tangent, pullback = jax.vjp(linear_map, perturbation.astype(jnp.float32))
    adjoint = pullback(adjoint_forcing.astype(jnp.float32))[0]
    return (tangent.astype(jnp.bfloat16), adjoint.astype(jnp.bfloat16))
```

```python
import functools
import jax
import jax.numpy as jnp
from jax import lax
from jax.experimental import pallas as pl
from jax.experimental.pallas import tpu as pltpu
from jax.sharding import PartitionSpec as P

POLAR_ROWS = 4
REACH = 2
HALO = 2
BANDS = 2 * REACH + 1
MESH = pl.DeviceIdType.MESH


def exchange(
    sizes,
    where_ref, own_ref, forcing_ref, onehot_ref, weights,
    tangent_ref, adjoint_ref,
    ext, contrib, spread, x_out, x_in, far_out, far_in, near_out, near_in,
    own_sem, z_send, z_recv, x_send, x_recv, ax_send, ax_recv, az_send, az_recv,
):
    lat_count, lon_count, rows, cols, stencil = sizes
    depth, cells = own_ref.shape[1], own_ref.shape[2]
    span = cols + 2 * HALO
    tile = rows * cols
    targets = tile
    picks = targets * stencil
    places = BANDS * span * rows
    half = cols // 2
    z = lax.axis_index("lat")
    x = lax.axis_index("lon")
    west = lax.rem(x + lon_count - 1, lon_count)
    east = lax.rem(x + 1, lon_count)
    polar = (z * rows < POLAR_ROWS) | ((z + 1) * rows > lat_count * rows - POLAR_ROWS)
    sides = ({"lon": west}, {"lon": east})
    steps = (1, -1)

    def there(offset):
        return (z + offset >= 0) & (z + offset < lat_count)

    def place(band, column):
        return ((band + REACH) * span + column) * rows

    barrier = pltpu.get_barrier_semaphore()
    for side in sides:
        pl.semaphore_signal(barrier, inc=1, device_id=side, device_id_type=MESH)
    for step in steps:
        @pl.when(there(step))
        def _():
            pl.semaphore_signal(barrier, inc=1, device_id={"lat": z + step}, device_id_type=MESH)

    own_copy = pltpu.make_async_copy(
        own_ref, ext.at[pl.ds(place(0, HALO), tile)], own_sem
    )
    own_copy.start()
    peers = len(sides) + (2 if lat_count > 2 else lat_count - 1)
    inner = there(1) & there(-1)

    @pl.when(inner)
    def _():
        pl.semaphore_wait(barrier, peers)

    @pl.when(jnp.logical_not(inner))
    def _():
        pl.semaphore_wait(barrier, peers - 1 if lat_count > 2 else peers)

    def z_copy(d, hop, part):
        source_band = -steps[d] if hop else 0
        band = -steps[d] * (hop + 1)
        offset = part * half
        size = half * rows
        if hop:
            src = ext.at[pl.ds(place(source_band, HALO + offset), size)]
        else:
            src = own_ref.at[pl.ds(offset * rows, size)]
        return pltpu.make_async_remote_copy(
            src_ref=src,
            dst_ref=ext.at[pl.ds(place(band, HALO + offset), size)],
            send_sem=z_send.at[d, hop, part],
            recv_sem=z_recv.at[d, hop, part],
            device_id={"lat": z + steps[d]},
            device_id_type=MESH,
        )

    def x_copy(band, side, j):
        mine = j if side == 0 else cols - 1 - j
        lands = cols + HALO + j if side == 0 else HALO - 1 - j
        if band == 0:
            src = own_ref.at[pl.ds(mine * rows, rows)]
        else:
            src = ext.at[pl.ds(place(band, HALO + mine), rows)]
        return pltpu.make_async_remote_copy(
            src_ref=src,
            dst_ref=ext.at[pl.ds(place(band, lands), rows)],
            send_sem=x_send.at[band + REACH, side, j],
            recv_sem=x_recv.at[band + REACH, side, j],
            device_id=sides[side],
            device_id_type=MESH,
        )

    def ax_copy(band, side, j):
        return pltpu.make_async_remote_copy(
            src_ref=x_out.at[band + REACH, side, j],
            dst_ref=x_in.at[band + REACH, side, j],
            send_sem=ax_send.at[band + REACH, side, j],
            recv_sem=ax_recv.at[band + REACH, side, j],
            device_id=sides[side],
            device_id_type=MESH,
        )

    def az_copy(d, near):
        return pltpu.make_async_remote_copy(
            src_ref=(near_out if near else far_out).at[d],
            dst_ref=(near_in if near else far_in).at[d],
            send_sem=az_send.at[d, near],
            recv_sem=az_recv.at[d, near],
            device_id={"lat": z + steps[d]},
            device_id_type=MESH,
        )

    def x_all(make, band, act):
        @pl.when(there(band))
        def _():
            for side in range(2):
                act(make(band, side, 0), band, side, 0)

            @pl.when(polar)
            def _():
                for side in range(2):
                    act(make(band, side, 1), band, side, 1)

    def start(copy, *_):
        copy.start()

    def wait_send(copy, *_):
        copy.wait_send()

    def wait_recv(copy, *_):
        copy.wait_recv()

    for d in range(2):
        @pl.when(there(steps[d]))
        def _():
            for part in range(2):
                z_copy(d, 0, part).start()
    x_all(x_copy, 0, start)

    def contribute(t, carry):
        block = weights[pl.ds(t * stencil, stencil)].reshape(stencil * cells, cells)
        part = lax.dot_general(
            forcing_ref[t], block, (((1,), (1,)), ((), ())), preferred_element_type=jnp.float32
        )
        for k in range(stencil):
            first = pl.multiple_of((t * stencil + k) * depth, depth)
            contrib[pl.ds(first, depth), :] = part[:, k * cells : (k + 1) * cells]
        return carry

    lax.fori_loop(0, targets, contribute, 0, unroll=2)

    def spread_rows(pair, carry):
        pieces = []
        for i in range(2):
            value = contrib[pl.ds(pair * 2 + i, picks, stride=depth), :]
            high = value.astype(jnp.bfloat16)
            low = (value - high.astype(jnp.float32)).astype(jnp.bfloat16)
            pieces.append(jnp.concatenate([high, low], axis=0))
        summed = jnp.dot(
            onehot_ref[...],
            jnp.concatenate(pieces, axis=1),
            preferred_element_type=jnp.float32,
        )
        for i in range(2):
            spread[pl.ds(pair * 2 + i, places, stride=depth), :] = summed[
                :, i * cells : (i + 1) * cells
            ]
        return carry

    lax.fori_loop(0, depth // 2, spread_rows, 0, unroll=2)

    def at(first, count):
        return pl.ds(first * depth, count * depth)

    def ax_start(copy, band, side, j):
        column = HALO - 1 - j if side == 0 else HALO + cols + j
        value = spread[at(place(band, column), rows), :].astype(jnp.bfloat16)
        x_out[band + REACH, side, j] = value.reshape(rows, depth, cells)
        copy.start()

    def ax_finish(copy, band, side, j):
        copy.wait_recv()
        column = HALO + cols - 1 - j if side == 0 else HALO + j
        here = at(place(band, column), rows)
        value = x_in[band + REACH, side, j].astype(jnp.float32)
        spread[here, :] += value.reshape(rows * depth, cells)

    for band in (2, -2):
        x_all(ax_copy, band, ax_start)
    for d in range(2):
        @pl.when(there(-steps[d]))
        def _():
            for part in range(2):
                z_copy(d, 0, part).wait_recv()

                @pl.when(there(steps[d]))
                def _():
                    z_copy(d, 1, part).start()
        x_all(x_copy, -steps[d], start)
    for band in (1, -1):
        x_all(ax_copy, band, ax_start)
    for d in range(2):
        @pl.when(there(-2 * steps[d]))
        def _():
            for part in range(2):
                z_copy(d, 1, part).wait_recv()
        x_all(x_copy, -2 * steps[d], start)
    x_all(ax_copy, 0, ax_start)

    for d in range(2):
        x_all(ax_copy, 2 * steps[d], ax_finish)

        @pl.when(there(2 * steps[d]))
        def _():
            value = spread[at(place(2 * steps[d], HALO), tile), :].astype(jnp.bfloat16)
            far_out[d] = value.reshape(tile, depth, cells)
            az_copy(d, 0).start()
    for d in range(2):
        x_all(ax_copy, steps[d], ax_finish)

        @pl.when(there(steps[d]))
        def _():
            here = at(place(steps[d], HALO), tile)

            @pl.when(there(-steps[d]))
            def _():
                az_copy(d, 0).wait_recv()
                spread[here, :] += far_in[d].astype(jnp.float32).reshape(tile * depth, cells)

            near_out[d] = spread[here, :].astype(jnp.bfloat16).reshape(tile, depth, cells)
            az_copy(d, 1).start()

    own_copy.wait()
    for band in range(-REACH, REACH + 1):
        x_all(x_copy, band, wait_recv)

    def interpolate(t, carry):
        sources = [ext[where_ref[t * stencil + k]] for k in range(stencil)]
        block = weights[pl.ds(t * stencil, stencil)].reshape(stencil * cells, cells)
        value = jnp.dot(
            jnp.concatenate(sources, axis=1), block, preferred_element_type=jnp.float32
        )
        tangent_ref[t] = value.astype(jnp.bfloat16)
        return carry

    lax.fori_loop(0, targets, interpolate, 0, unroll=2)

    x_all(ax_copy, 0, ax_finish)
    here = at(place(0, HALO), tile)
    for d in range(2):
        @pl.when(there(-steps[d]))
        def _():
            az_copy(d, 1).wait_recv()
            spread[here, :] += near_in[d].astype(jnp.float32).reshape(tile * depth, cells)
    adjoint_ref[...] = spread[here, :].astype(jnp.bfloat16).reshape(tile, depth, cells)

    for band in range(-REACH, REACH + 1):
        x_all(x_copy, band, wait_send)
        x_all(ax_copy, band, wait_send)
    for d in range(2):
        @pl.when(there(steps[d]))
        def _():
            for part in range(2):
                z_copy(d, 0, part).wait_send()
            az_copy(d, 1).wait_send()

            @pl.when(there(-steps[d]))
            def _():
                for part in range(2):
                    z_copy(d, 1, part).wait_send()

        @pl.when(there(2 * steps[d]))
        def _():
            az_copy(d, 0).wait_send()


def on_device(perturbation, adjoint_forcing, source_rows, source_cols, cubic_weights):
    fields, levels, rows, cols, cells = perturbation.shape
    stencil = source_rows.shape[2]
    depth = fields * levels
    span = cols + 2 * HALO
    tile = rows * cols
    picks = tile * stencil
    places = BANDS * span * rows
    lat_count = lax.axis_size("lat")
    lon_count = lax.axis_size("lon")
    z = lax.axis_index("lat")
    x = lax.axis_index("lon")
    local_rows = source_rows - z * rows + REACH * rows
    local_cols = jnp.mod(source_cols - x * cols + HALO, cols * lon_count)
    where = ((local_rows // rows) * span + local_cols) * rows + local_rows % rows
    where = where.reshape(picks).astype(jnp.int32)
    onehot = jnp.arange(places, dtype=jnp.int32)[:, None] == jnp.tile(where, 2)[None, :]
    onehot = onehot.astype(jnp.bfloat16)
    own = perturbation.transpose(3, 2, 0, 1, 4).reshape(tile, depth, cells)
    forcing = adjoint_forcing.transpose(2, 3, 0, 1, 4).reshape(tile, depth, cells)
    weights = cubic_weights.reshape(picks, cells, cells)

    vmem = pl.BlockSpec(memory_space=pltpu.VMEM)
    dma = pltpu.SemaphoreType.DMA
    bf16, f32 = jnp.bfloat16, jnp.float32
    tangent, adjoint = pl.pallas_call(
        functools.partial(exchange, (lat_count, lon_count, rows, cols, stencil)),
        name="exchange",
        out_shape=(
            jax.ShapeDtypeStruct((tile, depth, cells), bf16),
            jax.ShapeDtypeStruct((tile, depth, cells), bf16),
        ),
        in_specs=[
            pl.BlockSpec(memory_space=pltpu.SMEM),
            vmem,
            vmem,
            vmem,
            vmem,
        ],
        out_specs=(vmem, vmem),
        scratch_shapes=[
            pltpu.VMEM((places, depth, cells), bf16),
            pltpu.VMEM((picks * depth, cells), f32),
            pltpu.VMEM((places * depth, cells), f32),
            pltpu.VMEM((BANDS, 2, 2, rows, depth, cells), bf16),
            pltpu.VMEM((BANDS, 2, 2, rows, depth, cells), bf16),
            pltpu.VMEM((2, tile, depth, cells), bf16),
            pltpu.VMEM((2, tile, depth, cells), bf16),
            pltpu.VMEM((2, tile, depth, cells), bf16),
            pltpu.VMEM((2, tile, depth, cells), bf16),
            dma,
            dma((2, 2, 2)),
            dma((2, 2, 2)),
            dma((BANDS, 2, 2)),
            dma((BANDS, 2, 2)),
            dma((BANDS, 2, 2)),
            dma((BANDS, 2, 2)),
            dma((2, 2)),
            dma((2, 2)),
        ],
        compiler_params=pltpu.CompilerParams(
            collective_id=0, has_side_effects=True, vmem_limit_bytes=48 * 1024 * 1024
        ),
    )(where, own, forcing, onehot, weights)

    tangent_out = tangent.reshape(rows, cols, fields, levels, cells).transpose(2, 3, 0, 1, 4)
    adjoint_out = adjoint.reshape(cols, rows, fields, levels, cells).transpose(2, 3, 1, 0, 4)
    return (tangent_out, adjoint_out)


def solution(mesh):
    placed = (
        P("member", "lev", "lat", "lon", None),
        P("member", "lev", "lat", "lon", None),
        P("lat", "lon", None),
        P("lat", "lon", None),
        P("lat", "lon", None, None, None),
    )
    return jax.shard_map(
        on_device,
        mesh=mesh,
        in_specs=placed,
        out_specs=(P("member", "lev", "lat", "lon", None), P("member", "lev", "lat", "lon", None)),
        check_vma=False,
    )
```

```python
import functools
import jax
import jax.numpy as jnp
from jax import lax
from jax.experimental import pallas as pl
from jax.experimental.pallas import tpu as pltpu
from jax.sharding import PartitionSpec as P

POLAR_ROWS = 4
REACH = 2
HALO = 2
BANDS = 2 * REACH + 1
MESH = pl.DeviceIdType.MESH


def exchange(
    sizes,
    where_ref, own_ref, forcing_ref, onehot_ref, weights_hbm,
    tangent_ref, adjoint_ref,
    ext, weights, contrib, spread, x_out, x_in, lent, far_out, far_in, near_out, near_in,
    weight_sem, own_sem, fwd_send, fwd_recv, lend_send, lend_recv, z_send, z_recv, x_send, x_recv, ax_send, ax_recv, az_send, az_recv,
):
    lat_count, lon_count, rows, cols, stencil = sizes
    depth, cells = own_ref.shape[1], own_ref.shape[2]
    span = cols + 2 * HALO
    tile = rows * cols
    targets = tile
    picks = targets * stencil
    places = BANDS * span * rows
    half = cols // 2
    z = lax.axis_index("lat")
    x = lax.axis_index("lon")
    west = lax.rem(x + lon_count - 1, lon_count)
    east = lax.rem(x + 1, lon_count)
    polar = (z * rows < POLAR_ROWS) | ((z + 1) * rows > lat_count * rows - POLAR_ROWS)
    sides = ({"lon": west}, {"lon": east})
    steps = (1, -1)

    def there(offset):
        return (z + offset >= 0) & (z + offset < lat_count)

    def place(band, column):
        return ((band + REACH) * span + column) * rows

    barrier = pltpu.get_barrier_semaphore()
    for side in sides:
        pl.semaphore_signal(barrier, inc=1, device_id=side, device_id_type=MESH)
    for step in steps:
        @pl.when(there(step))
        def _():
            pl.semaphore_signal(barrier, inc=1, device_id={"lat": z + step}, device_id_type=MESH)

    weight_copy = pltpu.make_async_copy(weights_hbm, weights, weight_sem)
    weight_copy.start()
    own_copy = pltpu.make_async_copy(
        own_ref, ext.at[pl.ds(place(0, HALO), tile)], own_sem
    )
    own_copy.start()
    peers = len(sides) + (2 if lat_count > 2 else lat_count - 1)
    inner = there(1) & there(-1)

    @pl.when(inner)
    def _():
        pl.semaphore_wait(barrier, peers)

    @pl.when(jnp.logical_not(inner))
    def _():
        pl.semaphore_wait(barrier, peers - 1 if lat_count > 2 else peers)

    def z_copy(d, hop, part):
        source_band = -steps[d] if hop else 0
        band = -steps[d] * (hop + 1)
        offset = part * half
        size = half * rows
        if hop:
            src = ext.at[pl.ds(place(source_band, HALO + offset), size)]
        else:
            src = own_ref.at[pl.ds(offset * rows, size)]
        return pltpu.make_async_remote_copy(
            src_ref=src,
            dst_ref=ext.at[pl.ds(place(band, HALO + offset), size)],
            send_sem=z_send.at[d, hop, part],
            recv_sem=z_recv.at[d, hop, part],
            device_id={"lat": z + steps[d]},
            device_id_type=MESH,
        )

    def x_copy(band, side, j):
        mine = j if side == 0 else cols - 1 - j
        lands = cols + HALO + j if side == 0 else HALO - 1 - j
        if band == 0:
            src = own_ref.at[pl.ds(mine * rows, rows)]
        else:
            src = ext.at[pl.ds(place(band, HALO + mine), rows)]
        return pltpu.make_async_remote_copy(
            src_ref=src,
            dst_ref=ext.at[pl.ds(place(band, lands), rows)],
            send_sem=x_send.at[band + REACH, side, j],
            recv_sem=x_recv.at[band + REACH, side, j],
            device_id=sides[side],
            device_id_type=MESH,
        )

    def ax_copy(band, side, j):
        return pltpu.make_async_remote_copy(
            src_ref=x_out.at[band + REACH, side, j],
            dst_ref=x_in.at[band + REACH, side, j],
            send_sem=ax_send.at[band + REACH, side, j],
            recv_sem=ax_recv.at[band + REACH, side, j],
            device_id=sides[side],
            device_id_type=MESH,
        )

    def az_copy(d, near):
        return pltpu.make_async_remote_copy(
            src_ref=(near_out if near else far_out).at[d],
            dst_ref=(near_in if near else far_in).at[d],
            send_sem=az_send.at[d, near],
            recv_sem=az_recv.at[d, near],
            device_id={"lat": z + steps[d]},
            device_id_type=MESH,
        )

    lending = lat_count >= 4
    poles = ((0, 1), (lat_count - 1, -1)) if lending else ()

    def fwd_copy(pole, step, i, side):
        column = HALO + cols if side == 0 else HALO - 1
        return pltpu.make_async_remote_copy(
            src_ref=ext.at[pl.ds(place(i * step, column), rows)],
            dst_ref=ext.at[pl.ds(place((i + 1) * step, column), rows)],
            send_sem=fwd_send.at[i, side],
            recv_sem=fwd_recv.at[i, side],
            device_id={"lat": pole},
            device_id_type=MESH,
        )

    def lend_copy(pole, step, i, side):
        return pltpu.make_async_remote_copy(
            src_ref=x_out.at[(i + 1) * step + REACH, side, 0],
            dst_ref=lent.at[i, side],
            send_sem=lend_send.at[i, side],
            recv_sem=lend_recv.at[i, side],
            device_id={"lat": pole + step},
            device_id_type=MESH,
        )

    def x_all(make, band, act, which=(0, 1)):
        @pl.when(there(band))
        def _():
            def edge():
                for side in range(2):
                    act(make(band, side, 0), band, side, 0)

            if 0 in which:
                if band != 0 and lending:
                    pl.when(jnp.logical_not(polar))(edge)
                else:
                    edge()
            if 1 in which:
                @pl.when(polar)
                def _():
                    for side in range(2):
                        act(make(band, side, 1), band, side, 1)

    def start(copy, *_):
        copy.start()

    def wait_send(copy, *_):
        copy.wait_send()

    def wait_recv(copy, *_):
        copy.wait_recv()

    for d in range(2):
        @pl.when(there(steps[d]))
        def _():
            for part in range(2):
                z_copy(d, 0, part).start()
    x_all(x_copy, 0, start)

    weight_copy.wait()

    def contribute(t, carry):
        block = weights[pl.ds(t * stencil, stencil)].reshape(stencil * cells, cells)
        part = lax.dot_general(
            forcing_ref[t], block, (((1,), (1,)), ((), ())), preferred_element_type=jnp.float32
        )
        for k in range(stencil):
            first = pl.multiple_of((t * stencil + k) * depth, depth)
            contrib[pl.ds(first, depth), :] = part[:, k * cells : (k + 1) * cells]
        return carry

    lax.fori_loop(0, targets, contribute, 0, unroll=2)

    def spread_rows(pair, carry):
        pieces = []
        for i in range(2):
            value = contrib[pl.ds(pair * 2 + i, picks, stride=depth), :]
            high = value.astype(jnp.bfloat16)
            low = (value - high.astype(jnp.float32)).astype(jnp.bfloat16)
            pieces.append(jnp.concatenate([high, low], axis=0))
        summed = jnp.dot(
            onehot_ref[...],
            jnp.concatenate(pieces, axis=1),
            preferred_element_type=jnp.float32,
        )
        for i in range(2):
            spread[pl.ds(pair * 2 + i, places, stride=depth), :] = summed[
                :, i * cells : (i + 1) * cells
            ]
        return carry

    lax.fori_loop(0, depth // 2, spread_rows, 0, unroll=2)

    def at(first, count):
        return pl.ds(first * depth, count * depth)

    def away(side, j):
        return HALO - 1 - j if side == 0 else HALO + cols + j

    def ax_start(copy, band, side, j):
        value = spread[at(place(band, away(side, j)), rows), :].astype(jnp.bfloat16)
        x_out[band + REACH, side, j] = value.reshape(rows, depth, cells)
        copy.start()

    def ax_finish(copy, band, side, j):
        copy.wait_recv()
        column = HALO + cols - 1 - j if side == 0 else HALO + j
        here = at(place(band, column), rows)
        value = x_in[band + REACH, side, j].astype(jnp.float32)
        spread[here, :] += value.reshape(rows * depth, cells)

    for pole, step in poles:
        @pl.when(z == pole)
        def _():
            for i in range(2):
                for side in range(2):
                    ax_start(lend_copy(pole, step, i, side), (i + 1) * step, side, 0)
    for band in (2, -2):
        x_all(ax_copy, band, ax_start)
    for d in range(2):
        @pl.when(there(-steps[d]))
        def _():
            for part in range(2):
                z_copy(d, 0, part).wait_recv()

                @pl.when(there(steps[d]))
                def _():
                    z_copy(d, 1, part).start()
        x_all(x_copy, -steps[d], start)
    x_all(x_copy, 0, wait_recv, (0,))
    for pole, step in poles:
        @pl.when(z == pole + step)
        def _():
            for side in range(2):
                fwd_copy(pole, step, 0, side).start()
            for i in range(2):
                for side in range(2):
                    lend_copy(pole, step, i, side).wait_recv()
                    here = at(place(i * step, away(side, 0)), rows)
                    value = lent[i, side].astype(jnp.float32)
                    spread[here, :] += value.reshape(rows * depth, cells)
    for band in (1, -1):
        x_all(ax_copy, band, ax_start)
    for d in range(2):
        @pl.when(there(-2 * steps[d]))
        def _():
            for part in range(2):
                z_copy(d, 1, part).wait_recv()
        x_all(x_copy, -2 * steps[d], start)
    x_all(ax_copy, 0, ax_start)
    for band in (1, -1):
        x_all(x_copy, band, wait_recv, (0,))
    for pole, step in poles:
        @pl.when(z == pole + step)
        def _():
            for side in range(2):
                fwd_copy(pole, step, 1, side).start()

    for d in range(2):
        x_all(ax_copy, 2 * steps[d], ax_finish)

        @pl.when(there(2 * steps[d]))
        def _():
            value = spread[at(place(2 * steps[d], HALO), tile), :].astype(jnp.bfloat16)
            far_out[d] = value.reshape(tile, depth, cells)
            az_copy(d, 0).start()
    for d in range(2):
        x_all(ax_copy, steps[d], ax_finish)

        @pl.when(there(steps[d]))
        def _():
            here = at(place(steps[d], HALO), tile)

            @pl.when(there(-steps[d]))
            def _():
                az_copy(d, 0).wait_recv()
                spread[here, :] += far_in[d].astype(jnp.float32).reshape(tile * depth, cells)

            near_out[d] = spread[here, :].astype(jnp.bfloat16).reshape(tile, depth, cells)
            az_copy(d, 1).start()

    own_copy.wait()
    for band in range(-REACH, REACH + 1):
        x_all(x_copy, band, wait_recv, (0, 1) if abs(band) == 2 else (1,))
    for pole, step in poles:
        @pl.when(z == pole)
        def _():
            for i in range(2):
                for side in range(2):
                    fwd_copy(pole, step, i, side).wait_recv()

    def interpolate(t, carry):
        sources = [ext[where_ref[t * stencil + k]] for k in range(stencil)]
        block = weights[pl.ds(t * stencil, stencil)].reshape(stencil * cells, cells)
        value = jnp.dot(
            jnp.concatenate(sources, axis=1), block, preferred_element_type=jnp.float32
        )
        tangent_ref[t] = value.astype(jnp.bfloat16)
        return carry

    lax.fori_loop(0, targets, interpolate, 0, unroll=2)

    x_all(ax_copy, 0, ax_finish)
    here = at(place(0, HALO), tile)
    for d in range(2):
        @pl.when(there(-steps[d]))
        def _():
            az_copy(d, 1).wait_recv()
            spread[here, :] += near_in[d].astype(jnp.float32).reshape(tile * depth, cells)
    adjoint_ref[...] = spread[here, :].astype(jnp.bfloat16).reshape(tile, depth, cells)

    for band in range(-REACH, REACH + 1):
        x_all(x_copy, band, wait_send)
        x_all(ax_copy, band, wait_send)
    for pole, step in poles:
        for i in range(2):
            for side in range(2):
                @pl.when(z == pole)
                def _():
                    lend_copy(pole, step, i, side).wait_send()

                @pl.when(z == pole + step)
                def _():
                    fwd_copy(pole, step, i, side).wait_send()
    for d in range(2):
        @pl.when(there(steps[d]))
        def _():
            for part in range(2):
                z_copy(d, 0, part).wait_send()
            az_copy(d, 1).wait_send()

            @pl.when(there(-steps[d]))
            def _():
                for part in range(2):
                    z_copy(d, 1, part).wait_send()

        @pl.when(there(2 * steps[d]))
        def _():
            az_copy(d, 0).wait_send()


def on_device(perturbation, adjoint_forcing, source_rows, source_cols, cubic_weights):
    fields, levels, rows, cols, cells = perturbation.shape
    stencil = source_rows.shape[2]
    depth = fields * levels
    span = cols + 2 * HALO
    tile = rows * cols
    picks = tile * stencil
    places = BANDS * span * rows
    lat_count = lax.axis_size("lat")
    lon_count = lax.axis_size("lon")
    z = lax.axis_index("lat")
    x = lax.axis_index("lon")
    local_rows = source_rows - z * rows + REACH * rows
    local_cols = jnp.mod(source_cols - x * cols + HALO, cols * lon_count)
    where = ((local_rows // rows) * span + local_cols) * rows + local_rows % rows
    where = where.reshape(picks).astype(jnp.int32)
    onehot = jnp.arange(places, dtype=jnp.int32)[:, None] == jnp.tile(where, 2)[None, :]
    onehot = onehot.astype(jnp.bfloat16)
    own = perturbation.transpose(3, 2, 0, 1, 4).reshape(tile, depth, cells)
    forcing = adjoint_forcing.transpose(2, 3, 0, 1, 4).reshape(tile, depth, cells)
    weights = cubic_weights.reshape(picks, cells, cells)

    vmem = pl.BlockSpec(memory_space=pltpu.VMEM)
    dma = pltpu.SemaphoreType.DMA
    bf16, f32 = jnp.bfloat16, jnp.float32
    tangent, adjoint = pl.pallas_call(
        functools.partial(exchange, (lat_count, lon_count, rows, cols, stencil)),
        name="exchange",
        out_shape=(
            jax.ShapeDtypeStruct((tile, depth, cells), bf16),
            jax.ShapeDtypeStruct((tile, depth, cells), bf16),
        ),
        in_specs=[
            pl.BlockSpec(memory_space=pltpu.SMEM),
            vmem,
            vmem,
            vmem,
            pl.BlockSpec(memory_space=pltpu.HBM),
        ],
        out_specs=(vmem, vmem),
        scratch_shapes=[
            pltpu.VMEM((places, depth, cells), bf16),
            pltpu.VMEM((picks, cells, cells), bf16),
            pltpu.VMEM((picks * depth, cells), f32),
            pltpu.VMEM((places * depth, cells), f32),
            pltpu.VMEM((BANDS, 2, 2, rows, depth, cells), bf16),
            pltpu.VMEM((BANDS, 2, 2, rows, depth, cells), bf16),
            pltpu.VMEM((2, 2, rows, depth, cells), bf16),
            pltpu.VMEM((2, tile, depth, cells), bf16),
            pltpu.VMEM((2, tile, depth, cells), bf16),
            pltpu.VMEM((2, tile, depth, cells), bf16),
            pltpu.VMEM((2, tile, depth, cells), bf16),
            dma,
            dma,
            dma((2, 2)),
            dma((2, 2)),
            dma((2, 2)),
            dma((2, 2)),
            dma((2, 2, 2)),
            dma((2, 2, 2)),
            dma((BANDS, 2, 2)),
            dma((BANDS, 2, 2)),
            dma((BANDS, 2, 2)),
            dma((BANDS, 2, 2)),
            dma((2, 2)),
            dma((2, 2)),
        ],
        compiler_params=pltpu.CompilerParams(
            collective_id=0, has_side_effects=True, vmem_limit_bytes=48 * 1024 * 1024
        ),
    )(where, own, forcing, onehot, weights)

    tangent_out = tangent.reshape(rows, cols, fields, levels, cells).transpose(2, 3, 0, 1, 4)
    adjoint_out = adjoint.reshape(cols, rows, fields, levels, cells).transpose(2, 3, 1, 0, 4)
    return (tangent_out, adjoint_out)


def solution(mesh):
    placed = (
        P("member", "lev", "lat", "lon", None),
        P("member", "lev", "lat", "lon", None),
        P("lat", "lon", None),
        P("lat", "lon", None),
        P("lat", "lon", None, None, None),
    )
    return jax.shard_map(
        on_device,
        mesh=mesh,
        in_specs=placed,
        out_specs=(P("member", "lev", "lat", "lon", None), P("member", "lev", "lat", "lon", None)),
        check_vma=False,
    )
```

```python
import functools
import jax
import jax.numpy as jnp
from jax import lax
from jax.experimental import pallas as pl
from jax.experimental.pallas import tpu as pltpu
from jax.sharding import PartitionSpec as P

POLAR_ROWS = 4
REACH = 2
HALO = 2
BANDS = 2 * REACH + 1
MESH = pl.DeviceIdType.MESH


def exchange(
    sizes,
    where_ref, own_ref, forcing_ref, onehot_ref, weights_hbm,
    tangent_ref, adjoint_ref,
    ext, weights, contrib, spread, x_out, x_in, lent, far_out, far_in, near_out, near_in,
    weight_sem, own_sem, fwd_send, fwd_recv, lend_send, lend_recv, z_send, z_recv, x_send, x_recv, ax_send, ax_recv, az_send, az_recv,
):
    lat_count, lon_count, rows, cols, stencil = sizes
    depth, cells = own_ref.shape[1], own_ref.shape[2]
    span = cols + 2 * HALO
    tile = rows * cols
    targets = tile
    picks = targets * stencil
    places = BANDS * span * rows
    half = cols // 2
    z = lax.axis_index("lat")
    x = lax.axis_index("lon")
    west = lax.rem(x + lon_count - 1, lon_count)
    east = lax.rem(x + 1, lon_count)
    polar = (z * rows < POLAR_ROWS) | ((z + 1) * rows > lat_count * rows - POLAR_ROWS)
    sides = ({"lon": west}, {"lon": east})
    steps = (1, -1)

    def there(offset):
        return (z + offset >= 0) & (z + offset < lat_count)

    def place(band, column):
        return ((band + REACH) * span + column) * rows

    barrier = pltpu.get_barrier_semaphore()
    for side in sides:
        pl.semaphore_signal(barrier, inc=1, device_id=side, device_id_type=MESH)
    for step in steps:
        @pl.when(there(step))
        def _():
            pl.semaphore_signal(barrier, inc=1, device_id={"lat": z + step}, device_id_type=MESH)

    weight_copy = pltpu.make_async_copy(weights_hbm, weights, weight_sem)
    weight_copy.start()
    own_copy = pltpu.make_async_copy(
        own_ref, ext.at[pl.ds(place(0, HALO), tile)], own_sem
    )
    own_copy.start()
    peers = len(sides) + (2 if lat_count > 2 else lat_count - 1)
    inner = there(1) & there(-1)

    @pl.when(inner)
    def _():
        pl.semaphore_wait(barrier, peers)

    @pl.when(jnp.logical_not(inner))
    def _():
        pl.semaphore_wait(barrier, peers - 1 if lat_count > 2 else peers)

    def z_copy(d, hop, part):
        source_band = -steps[d] if hop else 0
        band = -steps[d] * (hop + 1)
        offset = part * half
        size = half * rows
        if hop:
            src = ext.at[pl.ds(place(source_band, HALO + offset), size)]
        else:
            src = own_ref.at[pl.ds(offset * rows, size)]
        return pltpu.make_async_remote_copy(
            src_ref=src,
            dst_ref=ext.at[pl.ds(place(band, HALO + offset), size)],
            send_sem=z_send.at[d, hop, part],
            recv_sem=z_recv.at[d, hop, part],
            device_id={"lat": z + steps[d]},
            device_id_type=MESH,
        )

    def x_copy(band, side, j):
        mine = j if side == 0 else cols - 1 - j
        lands = cols + HALO + j if side == 0 else HALO - 1 - j
        if band == 0:
            src = own_ref.at[pl.ds(mine * rows, rows)]
        else:
            src = ext.at[pl.ds(place(band, HALO + mine), rows)]
        return pltpu.make_async_remote_copy(
            src_ref=src,
            dst_ref=ext.at[pl.ds(place(band, lands), rows)],
            send_sem=x_send.at[band + REACH, side, j],
            recv_sem=x_recv.at[band + REACH, side, j],
            device_id=sides[side],
            device_id_type=MESH,
        )

    def ax_copy(band, side, j):
        return pltpu.make_async_remote_copy(
            src_ref=x_out.at[band + REACH, side, j],
            dst_ref=x_in.at[band + REACH, side, j],
            send_sem=ax_send.at[band + REACH, side, j],
            recv_sem=ax_recv.at[band + REACH, side, j],
            device_id=sides[side],
            device_id_type=MESH,
        )

    def az_copy(d, near, part):
        return pltpu.make_async_remote_copy(
            src_ref=(near_out if near else far_out).at[d, part],
            dst_ref=(near_in if near else far_in).at[d, part],
            send_sem=az_send.at[d, near, part],
            recv_sem=az_recv.at[d, near, part],
            device_id={"lat": z + steps[d]},
            device_id_type=MESH,
        )

    lending = lat_count >= 4
    poles = ((0, 1), (lat_count - 1, -1)) if lending else ()

    def fwd_copy(pole, step, i, side):
        column = HALO + cols if side == 0 else HALO - 1
        return pltpu.make_async_remote_copy(
            src_ref=ext.at[pl.ds(place(i * step, column), rows)],
            dst_ref=ext.at[pl.ds(place((i + 1) * step, column), rows)],
            send_sem=fwd_send.at[i, side],
            recv_sem=fwd_recv.at[i, side],
            device_id={"lat": pole},
            device_id_type=MESH,
        )

    def lend_copy(pole, step, i, side):
        return pltpu.make_async_remote_copy(
            src_ref=x_out.at[(i + 1) * step + REACH, side, 0],
            dst_ref=lent.at[i, side],
            send_sem=lend_send.at[i, side],
            recv_sem=lend_recv.at[i, side],
            device_id={"lat": pole + step},
            device_id_type=MESH,
        )

    def x_all(make, band, act, which=(0, 1)):
        @pl.when(there(band))
        def _():
            def edge():
                for side in range(2):
                    act(make(band, side, 0), band, side, 0)

            if 0 in which:
                if band != 0 and lending:
                    pl.when(jnp.logical_not(polar))(edge)
                else:
                    edge()
            if 1 in which:
                @pl.when(polar)
                def _():
                    for side in range(2):
                        act(make(band, side, 1), band, side, 1)

    def start(copy, *_):
        copy.start()

    def wait_send(copy, *_):
        copy.wait_send()

    def wait_recv(copy, *_):
        copy.wait_recv()

    for d in range(2):
        @pl.when(there(steps[d]))
        def _():
            for part in range(2):
                z_copy(d, 0, part).start()
    x_all(x_copy, 0, start)

    weight_copy.wait()

    def contribute(t, carry):
        block = weights[pl.ds(t * stencil, stencil)].reshape(stencil * cells, cells)
        part = lax.dot_general(
            forcing_ref[t], block, (((1,), (1,)), ((), ())), preferred_element_type=jnp.float32
        )
        for k in range(stencil):
            first = pl.multiple_of((t * stencil + k) * depth, depth)
            contrib[pl.ds(first, depth), :] = part[:, k * cells : (k + 1) * cells]
        return carry

    lax.fori_loop(0, targets, contribute, 0, unroll=2)

    def spread_rows(pair, carry):
        pieces = []
        for i in range(2):
            value = contrib[pl.ds(pair * 2 + i, picks, stride=depth), :]
            high = value.astype(jnp.bfloat16)
            low = (value - high.astype(jnp.float32)).astype(jnp.bfloat16)
            pieces.append(jnp.concatenate([high, low], axis=0))
        summed = jnp.dot(
            onehot_ref[...],
            jnp.concatenate(pieces, axis=1),
            preferred_element_type=jnp.float32,
        )
        for i in range(2):
            spread[pl.ds(pair * 2 + i, places, stride=depth), :] = summed[
                :, i * cells : (i + 1) * cells
            ]
        return carry

    lax.fori_loop(0, depth // 2, spread_rows, 0, unroll=2)

    def at(first, count):
        return pl.ds(first * depth, count * depth)

    def away(side, j):
        return HALO - 1 - j if side == 0 else HALO + cols + j

    def ax_start(copy, band, side, j):
        value = spread[at(place(band, away(side, j)), rows), :].astype(jnp.bfloat16)
        x_out[band + REACH, side, j] = value.reshape(rows, depth, cells)
        copy.start()

    def ax_finish(copy, band, side, j):
        copy.wait_recv()
        column = HALO + cols - 1 - j if side == 0 else HALO + j
        here = at(place(band, column), rows)
        value = x_in[band + REACH, side, j].astype(jnp.float32)
        spread[here, :] += value.reshape(rows * depth, cells)

    for pole, step in poles:
        @pl.when(z == pole)
        def _():
            for i in (1, 0):
                for side in range(2):
                    ax_start(lend_copy(pole, step, i, side), (i + 1) * step, side, 0)
    for band in (2, -2):
        x_all(ax_copy, band, ax_start)
    for d in range(2):
        @pl.when(there(-steps[d]))
        def _():
            for part in range(2):
                z_copy(d, 0, part).wait_recv()

                @pl.when(there(steps[d]))
                def _():
                    z_copy(d, 1, part).start()
        x_all(x_copy, -steps[d], start)

    borrows = {step: z == pole + step for pole, step in poles}
    for step in steps:
        if lending:
            @pl.when(jnp.logical_not(borrows[step]))
            def _():
                x_all(ax_copy, step, ax_start)
        else:
            x_all(ax_copy, step, ax_start)
    x_all(x_copy, 0, wait_recv, (0,))
    for pole, step in poles:
        @pl.when(z == pole + step)
        def _():
            for side in range(2):
                fwd_copy(pole, step, 0, side).start()

    for d in range(2):
        x_all(ax_copy, 2 * steps[d], ax_finish)

        @pl.when(there(2 * steps[d]))
        def _():
            for part in range(cols):
                here = at(place(2 * steps[d], HALO + part), rows)
                value = spread[here, :].astype(jnp.bfloat16)
                far_out[d, part] = value.reshape(rows, depth, cells)
                az_copy(d, 0, part).start()

    def borrow(pole, step, i):
        for side in range(2):
            lend_copy(pole, step, i, side).wait_recv()
            here = at(place(i * step, away(side, 0)), rows)
            value = lent[i, side].astype(jnp.float32)
            spread[here, :] += value.reshape(rows * depth, cells)

    for pole, step in poles:
        @pl.when(z == pole + step)
        def _():
            borrow(pole, step, 1)
            x_all(ax_copy, step, ax_start)
            borrow(pole, step, 0)
    x_all(ax_copy, 0, ax_start)

    for d in range(2):
        @pl.when(there(-2 * steps[d]))
        def _():
            for part in range(2):
                z_copy(d, 1, part).wait_recv()
        x_all(x_copy, -2 * steps[d], start)
    for band in (1, -1):
        x_all(x_copy, band, wait_recv, (0,))
    for pole, step in poles:
        @pl.when(z == pole + step)
        def _():
            for side in range(2):
                fwd_copy(pole, step, 1, side).start()

    for d in range(2):
        x_all(ax_copy, steps[d], ax_finish)

        @pl.when(there(steps[d]))
        def _():
            for part in range(cols):
                here = at(place(steps[d], HALO + part), rows)

                @pl.when(there(-steps[d]))
                def _():
                    az_copy(d, 0, part).wait_recv()
                    value = far_in[d, part].astype(jnp.float32)
                    spread[here, :] += value.reshape(rows * depth, cells)

                value = spread[here, :].astype(jnp.bfloat16)
                near_out[d, part] = value.reshape(rows, depth, cells)
                az_copy(d, 1, part).start()

    own_copy.wait()
    for band in range(-REACH, REACH + 1):
        x_all(x_copy, band, wait_recv, (0, 1) if abs(band) == 2 else (1,))
    for pole, step in poles:
        @pl.when(z == pole)
        def _():
            for i in range(2):
                for side in range(2):
                    fwd_copy(pole, step, i, side).wait_recv()

    def interpolate(t, carry):
        sources = [ext[where_ref[t * stencil + k]] for k in range(stencil)]
        block = weights[pl.ds(t * stencil, stencil)].reshape(stencil * cells, cells)
        value = jnp.dot(
            jnp.concatenate(sources, axis=1), block, preferred_element_type=jnp.float32
        )
        tangent_ref[t] = value.astype(jnp.bfloat16)
        return carry

    lax.fori_loop(0, targets, interpolate, 0, unroll=2)

    x_all(ax_copy, 0, ax_finish)
    here = at(place(0, HALO), tile)
    for d in range(2):
        @pl.when(there(-steps[d]))
        def _():
            for part in range(cols):
                az_copy(d, 1, part).wait_recv()
            spread[here, :] += near_in[d].astype(jnp.float32).reshape(tile * depth, cells)
    adjoint_ref[...] = spread[here, :].astype(jnp.bfloat16).reshape(tile, depth, cells)

    for band in range(-REACH, REACH + 1):
        x_all(x_copy, band, wait_send)
        x_all(ax_copy, band, wait_send)
    for pole, step in poles:
        for i in range(2):
            for side in range(2):
                @pl.when(z == pole)
                def _():
                    lend_copy(pole, step, i, side).wait_send()

                @pl.when(z == pole + step)
                def _():
                    fwd_copy(pole, step, i, side).wait_send()
    for d in range(2):
        @pl.when(there(steps[d]))
        def _():
            for part in range(2):
                z_copy(d, 0, part).wait_send()
            for part in range(cols):
                az_copy(d, 1, part).wait_send()

            @pl.when(there(-steps[d]))
            def _():
                for part in range(2):
                    z_copy(d, 1, part).wait_send()

        @pl.when(there(2 * steps[d]))
        def _():
            for part in range(cols):
                az_copy(d, 0, part).wait_send()


def on_device(perturbation, adjoint_forcing, source_rows, source_cols, cubic_weights):
    fields, levels, rows, cols, cells = perturbation.shape
    stencil = source_rows.shape[2]
    depth = fields * levels
    span = cols + 2 * HALO
    tile = rows * cols
    picks = tile * stencil
    places = BANDS * span * rows
    lat_count = lax.axis_size("lat")
    lon_count = lax.axis_size("lon")
    z = lax.axis_index("lat")
    x = lax.axis_index("lon")
    local_rows = source_rows - z * rows + REACH * rows
    local_cols = jnp.mod(source_cols - x * cols + HALO, cols * lon_count)
    where = ((local_rows // rows) * span + local_cols) * rows + local_rows % rows
    where = where.reshape(picks).astype(jnp.int32)
    onehot = jnp.arange(places, dtype=jnp.int32)[:, None] == jnp.tile(where, 2)[None, :]
    onehot = onehot.astype(jnp.bfloat16)
    own = perturbation.transpose(3, 2, 0, 1, 4).reshape(tile, depth, cells)
    forcing = adjoint_forcing.transpose(2, 3, 0, 1, 4).reshape(tile, depth, cells)
    weights = pltpu.with_memory_space_constraint(
        cubic_weights.reshape(picks, cells, cells), pltpu.HBM
    )

    vmem = pl.BlockSpec(memory_space=pltpu.VMEM)
    dma = pltpu.SemaphoreType.DMA
    bf16, f32 = jnp.bfloat16, jnp.float32
    tangent, adjoint = pl.pallas_call(
        functools.partial(exchange, (lat_count, lon_count, rows, cols, stencil)),
        name="exchange",
        out_shape=(
            jax.ShapeDtypeStruct((tile, depth, cells), bf16),
            jax.ShapeDtypeStruct((tile, depth, cells), bf16),
        ),
        in_specs=[
            pl.BlockSpec(memory_space=pltpu.SMEM),
            vmem,
            vmem,
            vmem,
            pl.BlockSpec(memory_space=pltpu.HBM),
        ],
        out_specs=(vmem, vmem),
        scratch_shapes=[
            pltpu.VMEM((places, depth, cells), bf16),
            pltpu.VMEM((picks, cells, cells), bf16),
            pltpu.VMEM((picks * depth, cells), f32),
            pltpu.VMEM((places * depth, cells), f32),
            pltpu.VMEM((BANDS, 2, 2, rows, depth, cells), bf16),
            pltpu.VMEM((BANDS, 2, 2, rows, depth, cells), bf16),
            pltpu.VMEM((2, 2, rows, depth, cells), bf16),
            pltpu.VMEM((2, cols, rows, depth, cells), bf16),
            pltpu.VMEM((2, cols, rows, depth, cells), bf16),
            pltpu.VMEM((2, cols, rows, depth, cells), bf16),
            pltpu.VMEM((2, cols, rows, depth, cells), bf16),
            dma,
            dma,
            dma((2, 2)),
            dma((2, 2)),
            dma((2, 2)),
            dma((2, 2)),
            dma((2, 2, 2)),
            dma((2, 2, 2)),
            dma((BANDS, 2, 2)),
            dma((BANDS, 2, 2)),
            dma((BANDS, 2, 2)),
            dma((BANDS, 2, 2)),
            dma((2, 2, cols)),
            dma((2, 2, cols)),
        ],
        compiler_params=pltpu.CompilerParams(
            collective_id=0, has_side_effects=True, vmem_limit_bytes=48 * 1024 * 1024
        ),
    )(where, own, forcing, onehot, weights)

    tangent_out = tangent.reshape(rows, cols, fields, levels, cells).transpose(2, 3, 0, 1, 4)
    adjoint_out = adjoint.reshape(cols, rows, fields, levels, cells).transpose(2, 3, 1, 0, 4)
    return (tangent_out, adjoint_out)


def solution(mesh):
    placed = (
        P("member", "lev", "lat", "lon", None),
        P("member", "lev", "lat", "lon", None),
        P("lat", "lon", None),
        P("lat", "lon", None),
        P("lat", "lon", None, None, None),
    )
    return jax.shard_map(
        on_device,
        mesh=mesh,
        in_specs=placed,
        out_specs=(P("member", "lev", "lat", "lon", None), P("member", "lev", "lat", "lon", None)),
        check_vma=False,
    )
```
